32 devices in a mesh: rows: 4 (over z), cols: 2 (over x), slabs: 4 (over y, core).
Axes of the slice: x: 2, y: 2, z: 4, core: 2. Of those that a mesh axis runs over, the one named last changes fastest.
Arguments:
- pressure: float32 [512, 8, 128, 128], P('rows', 'cols', 'slabs'), may hold values from 0.5 to 2
- earlier: float32 [512, 8, 128, 128], P('rows', 'cols', 'slabs'), may hold values from 0.2 to 1.8
- speed_square: float32 [512, 8, 128, 128], P('rows', 'cols', 'slabs'), may hold values from 0.05 to 0.3
Outputs:
- scaled_field: float32 [512, 8, 128, 128], P('rows', 'cols', 'slabs')
- pressure_end: float32 [512, 8, 128, 128], P('rows', 'cols', 'slabs')
The draws below stay inside these ranges and needn't reach their ends.
All inputs are finite; a program needn't handle non-finite values.
Results may differ from the reference program's by a relative error of at most 0.00002.
Values sent between devices are 32-bit elements; how exact they have to be, the bound alone decides.
No kernel may reach another device: no remote copies, remote signals or barrier semaphores. Data moves between devices by JAX's collectives and lax.ppermute only.
A program may use at most 128 MiB of HBM per device.

```python
import jax
import jax.numpy as jnp
from jax import lax

GRID_J = 512
GRID_I = 8
GRID_K = 128
MEMBERS = 128
STEPS = 3


def block_scale(key, extent, pieces, least, top_value):
    loudness, own = 1.0, jax.random.fold_in(key, 6)
    for position, blocks in pieces:
        heights = jnp.exp(jax.random.uniform(jax.random.fold_in(own, position), (blocks,), jnp.float32, least / len(pieces), top_value / len(pieces)))
        loudness = loudness * jnp.repeat(heights, extent[position] // blocks).reshape([-1 if axis == position else 1 for axis in range(len(extent))])
    return loudness


def setup_inputs(seed: int = 0) -> dict:
    streams_of = jax.random.split(jax.random.key(seed), 4)
    pressure = jnp.clip(0.5 + 1.5 * jax.random.uniform(streams_of[0], (GRID_J, GRID_I, GRID_K, MEMBERS), jnp.float32) ** block_scale(streams_of[0], (GRID_J, GRID_I, GRID_K, MEMBERS), ((0, 4), (1, 2), (2, 4)), -0.2, 0.2), 0.5, 2.0)
    earlier = jnp.clip(0.2 + 1.5999999 * jax.random.uniform(streams_of[1], (GRID_J, GRID_I, GRID_K, MEMBERS), jnp.float32) ** block_scale(streams_of[1], (GRID_J, GRID_I, GRID_K, MEMBERS), ((0, 4), (1, 2), (2, 4)), -0.2, 0.2), 0.2, 1.8)
    speed_square = jnp.clip(0.05 + 0.25 * jax.random.uniform(streams_of[2], (GRID_J, GRID_I, GRID_K, MEMBERS), jnp.float32) ** block_scale(streams_of[2], (GRID_J, GRID_I, GRID_K, MEMBERS), ((0, 4), (1, 2), (2, 4)), -0.2, 0.2), 0.05, 0.3)
    return dict(pressure=pressure, earlier=earlier, speed_square=speed_square)


def strip_edges(values, dims):
    for dim in dims:
        values = lax.slice_in_dim(values, 1, values.shape[dim] - 1, axis=dim)
    return values

def neighbour(values, dim, start, dims):
    others = [other for other in dims if other != dim]
    values = strip_edges(values, others)
    return lax.slice_in_dim(values, start, start + values.shape[dim] - 2, axis=dim)

def one_step(padded, before, speed_square):
    middle = strip_edges(padded, (0, 1, 2))
    lower = [neighbour(padded, dim, 0, (0, 1, 2)) for dim in (0, 1, 2)]
    upper = [neighbour(padded, dim, 2, (0, 1, 2)) for dim in (0, 1, 2)]
    spread = lower[0] + upper[0] + lower[1] + upper[1] + lower[2] + upper[2] - 6.0 * middle
    return 2.0 * middle - before + speed_square * spread

def reference(pressure, earlier, speed_square):
    for step in range(STEPS):
        later = one_step(jnp.pad(pressure, ((1, 1), (1, 1), (1, 1), (0, 0)), mode='wrap'), earlier, speed_square)
        earlier, pressure = (pressure, later)
    line_mean = lax.optimization_barrier(jnp.mean(pressure, axis=0, keepdims=True))
    centred = pressure - line_mean
    line_variance = lax.optimization_barrier(jnp.mean(centred * centred, axis=0, keepdims=True))
    scaled_field = centred * lax.rsqrt(line_variance + 0.0001)
    return (scaled_field, pressure)
```

```python
import functools

import jax
import jax.numpy as jnp
from jax import lax
from jax.experimental import pallas as pl
from jax.experimental.pallas import tpu as pltpu
from jax.sharding import PartitionSpec as P

STEPS = 3


def shift(values, axis, by):
    count = lax.axis_size(axis)
    return lax.ppermute(values, axis, [(i, (i + by) % count) for i in range(count)])


def block_rows(rows):
    for size in (32, 16, 8):
        if rows % size == 0:
            return size
    return rows


def blocked(operand, rows):
    array, index = operand
    tail = array.shape[-2:]
    if index is None:
        return pl.BlockSpec((rows, *tail), lambda j: (j, 0, 0))
    return pl.BlockSpec((rows, None, *tail), lambda j: (j, index, 0, 0))


def whole(operand):
    array, index = operand
    tail = array.shape[-2:]
    if index is None:
        return pl.BlockSpec((array.shape[0], *tail), lambda j: (0, 0, 0))
    return pl.BlockSpec((array.shape[0], None, *tail), lambda j: (0, index, 0, 0))


def edge(operand):
    array, index = operand
    if index is None:
        return pl.BlockSpec(array.shape, lambda j: (0, 0))
    return pl.BlockSpec((None, *array.shape[1:]), lambda j: (index, 0, 0))


def updated_row(refs, start, j):
    mid, low, up, before, speed, k_low, k_high, j_low, j_high = refs
    total = mid.shape[0]
    row = start + j
    here = mid[row]
    length = here.shape[0]
    position = lax.broadcasted_iota(jnp.int32, here.shape, 0)
    earlier_j = jnp.where(row == 0, j_low[...], mid[jnp.maximum(row - 1, 0)])
    later_j = jnp.where(row == total - 1, j_high[...], mid[jnp.minimum(row + 1, total - 1)])
    lower_k = jnp.where(position == 0, k_low[pl.ds(row, 1), :], pltpu.roll(here, 1, 0))
    upper_k = jnp.where(position == length - 1, k_high[pl.ds(row, 1), :], pltpu.roll(here, length - 1, 0))
    spread = earlier_j + later_j + low[j] + up[j] + lower_k + upper_k - 6.0 * here
    return 2.0 * here - before[j] + speed[j] * spread


def step_kernel(*refs, rows):
    ins, (out, k_first, k_last, j_first, j_last) = refs[:9], refs[9:]
    block = pl.program_id(0)
    start = block * rows

    def body(j, carry):
        new = updated_row(ins, start, j)
        out[j] = new
        k_first[pl.ds(j, 1), :] = new[:1]
        k_last[pl.ds(j, 1), :] = new[new.shape[0] - 1 :]
        return carry

    lax.fori_loop(0, rows, body, 0, unroll=4)

    @pl.when(block == 0)
    def _():
        j_first[...] = out[0]

    @pl.when(block == pl.num_programs(0) - 1)
    def _():
        j_last[...] = out[rows - 1]


def last_kernel(*refs, rows, aliased):
    ins = refs[:9]
    out, field, stats, guess, total, square = refs[9 + aliased :]
    block = pl.program_id(0)
    start = block * rows

    @pl.when(block == 0)
    def _():
        guess[...] = updated_row(ins, start, 0)
        total[...] = jnp.zeros_like(total)
        square[...] = jnp.zeros_like(square)

    base = guess[...]

    def body(j, carry):
        sums, squares = carry
        new = updated_row(ins, start, j)
        out[j] = new
        field[j] = new
        moved = new - base
        return sums + moved, squares + moved * moved

    sums, squares = lax.fori_loop(0, rows, body, (total[...], square[...]), unroll=4)
    total[...] = sums
    square[...] = squares

    @pl.when(block == pl.num_programs(0) - 1)
    def _():
        count = rows * pl.num_programs(0)
        mean = sums / count
        stats[0] = base + mean
        stats[1] = jnp.maximum(squares - sums * mean, 0.0)


def scale_kernel(*refs):
    values, mean, factor = refs[:3]
    out = refs[-1]

    def body(j, carry):
        out[j] = (values[j] - mean[...]) * factor[...]
        return carry

    lax.fori_loop(0, values.shape[0], body, 0, unroll=4)


def cost(microseconds):
    return pl.CostEstimate(flops=int(microseconds * 1.0e9), bytes_accessed=12 << 20, transcendentals=0)


def plane_specs(mid, low, up, before, speed, edges, rows):
    operands = [mid, low, up, before, speed, *edges]
    specs = [whole(mid)] + [blocked(o, rows) for o in operands[1:5]] + [edge(o) for o in edges]
    return [array for array, _ in operands], specs


def plane_step(name, mid, low, up, before, speed, edges):
    nj, nk, members = mid[0].shape[0], *mid[0].shape[-2:]
    rows = block_rows(nj)
    arrays, specs = plane_specs(mid, low, up, before, speed, edges, rows)
    plane = pl.BlockSpec((rows, nk, members), lambda j: (j, 0, 0))
    k_edge = pl.BlockSpec((rows, members), lambda j: (j, 0))
    j_edge = pl.BlockSpec((nk, members), lambda j: (0, 0))
    shape = functools.partial(jax.ShapeDtypeStruct, dtype=jnp.float32)
    return pl.pallas_call(
        functools.partial(step_kernel, rows=rows),
        grid=(nj // rows,),
        in_specs=specs,
        out_specs=[plane, k_edge, k_edge, j_edge, j_edge],
        out_shape=[shape((nj, nk, members)), shape((nj, members)), shape((nj, members)), shape((nk, members)), shape((nk, members))],
        cost_estimate=cost(8),
        name=name,
    )(*arrays)


def plane_last(name, mid, low, up, before, speed, edges, field, index, field_shape):
    nj, nk, members = mid[0].shape[0], *mid[0].shape[-2:]
    rows = block_rows(nj)
    arrays, specs = plane_specs(mid, low, up, before, speed, edges, rows)
    shape = functools.partial(jax.ShapeDtypeStruct, dtype=jnp.float32)
    aliases = {}
    if field is not None:
        aliases = {len(arrays): 1}
        arrays.append(field)
        specs.append(pl.BlockSpec(memory_space=pl.ANY))
    return pl.pallas_call(
        functools.partial(last_kernel, rows=rows, aliased=len(aliases)),
        grid=(nj // rows,),
        in_specs=specs,
        out_specs=[
            pl.BlockSpec((rows, nk, members), lambda j: (j, 0, 0)),
            pl.BlockSpec((rows, None, nk, members), lambda j: (j, index, 0, 0)),
            pl.BlockSpec((2, nk, members), lambda j: (0, 0, 0)),
        ],
        out_shape=[shape((nj, nk, members)), shape(field_shape), shape((2, nk, members))],
        scratch_shapes=[pltpu.VMEM((nk, members), jnp.float32)] * 3,
        input_output_aliases=aliases,
        cost_estimate=cost(8),
        name=name,
    )(*arrays)


def plane_scale(name, values, mean, factor, scaled, index, field_shape):
    nj, nk, members = values.shape
    rows = block_rows(nj)
    arrays = [values, mean, factor]
    line = pl.BlockSpec((nk, members), lambda j: (0, 0))
    specs = [pl.BlockSpec((rows, nk, members), lambda j: (j, 0, 0)), line, line]
    aliases = {}
    if scaled is not None:
        aliases = {3: 0}
        arrays.append(scaled)
        specs.append(pl.BlockSpec(memory_space=pl.ANY))
    return pl.pallas_call(
        scale_kernel,
        grid=(nj // rows,),
        in_specs=specs,
        out_specs=pl.BlockSpec((rows, None, nk, members), lambda j: (j, index, 0, 0)),
        out_shape=jax.ShapeDtypeStruct(field_shape, jnp.float32),
        input_output_aliases=aliases,
        cost_estimate=cost(4),
        name=name,
    )(*arrays)


def exchanged(k_first, k_last, j_first, j_last):
    return (shift(k_last, "slabs", 1), shift(k_first, "slabs", -1), shift(j_last, "rows", 1), shift(j_first, "rows", -1))


def line_factors(stats, local):
    count = lax.axis_size("rows")
    parts = [stats] + [shift(stats, "rows", by) for by in range(1, count)]
    mean = sum(part[0] for part in parts) / count
    spread = sum(part[1] for part in parts) / (local * count)
    spread = spread + sum((part[0] - mean) ** 2 for part in parts) / count
    return mean, lax.rsqrt(spread + 0.0001)


def shards(pressure, earlier, speed_square):
    nj, ni, nk, members = pressure.shape
    top = ni - 1
    inner = range(1, top)
    now = [(pressure, i) for i in range(ni)]
    before = [(earlier, i) for i in range(ni)]
    speed = [(speed_square, i) for i in range(ni)]
    first_top = shift(pressure[:, top], "cols", 1)
    first_bottom = shift(pressure[:, 0], "cols", -1)
    received = {"low": first_top, "up": first_bottom}
    swap = lambda values: jnp.transpose(values, (1, 0, 2))
    halos = exchanged(swap(pressure[:, :, 0]), swap(pressure[:, :, nk - 1]), pressure[0], pressure[nj - 1])
    edges = [[(h, i) for h in halos] for i in range(ni)]
    for step in range(STEPS - 1):
        order = (0, top) if step % 2 == 0 else (top, 0)
        later, new_edges, arriving = [None] * ni, [None] * ni, {}
        ready = [None] * ni

        def compute(i):
            low = (received["low"], None) if i == 0 else now[i - 1]
            up = (received["up"], None) if i == top else now[i + 1]
            ready[i] = plane_step(f"step{step}_plane{i}", now[i], low, up, before[i], speed[i], edges[i])
            later[i] = (ready[i][0], None)

        for i in inner:
            compute(i)
        stacked = exchanged(*[jnp.stack([ready[i][n] for i in inner]) for n in range(1, 5)])
        for i in inner:
            new_edges[i] = [(h, i - 1) for h in stacked]
        for i in order:
            compute(i)
            if i == 0:
                arriving["up"] = shift(ready[i][0], "cols", -1)
            else:
                arriving["low"] = shift(ready[i][0], "cols", 1)
            new_edges[i] = [(h, None) for h in exchanged(*ready[i][1:])]
        before, now, edges, received = now, later, new_edges, arriving
    order = (0, top) if STEPS % 2 == 1 else (top, 0)
    field = scaled = None
    for i in (*inner, *order):
        low = (received["low"], None) if i == 0 else now[i - 1]
        up = (received["up"], None) if i == top else now[i + 1]
        values, field, stats = plane_last(f"last_plane{i}", now[i], low, up, before[i], speed[i], edges[i], field, i, pressure.shape)
        mean, factor = line_factors(stats, nj)
        scaled = plane_scale(f"scale_plane{i}", values, mean, factor, scaled, i, pressure.shape)
    return (scaled, field)


def solution(mesh):
    spec = P("rows", "cols", "slabs", None)
    return jax.shard_map(shards, mesh=mesh, in_specs=(spec,) * 3, out_specs=(spec,) * 2, check_vma=False)
```

```python
import functools

import jax
import jax.numpy as jnp
from jax import lax
from jax.experimental import pallas as pl
from jax.experimental.pallas import tpu as pltpu
from jax.sharding import PartitionSpec as P

STEPS = 3


def shift(values, axis, by):
    count = lax.axis_size(axis)
    return lax.ppermute(values, axis, [(i, (i + by) % count) for i in range(count)])


def block_rows(rows):
    for size in (32, 16, 8):
        if rows % size == 0:
            return size
    return rows


def pieces(length):
    if length % 32 == 0:
        half, quarter = length // 2, length // 4
        return ((0, half), (half, quarter), (half + quarter, quarter))
    return ((0, length),)


def blocked(operand, rows, piece):
    array, index = operand
    start, length = piece
    members = array.shape[-1]
    k = 0 if array.shape[-2] == length else start // length
    if index is None:
        return pl.BlockSpec((rows, length, members), lambda j: (j, k, 0))
    return pl.BlockSpec((rows, None, length, members), lambda j: (j, index, k, 0))


def window(piece, total):
    start, length = piece
    if start % (2 * length) == length and start + length == total:
        return (start - length, 2 * length)
    return (0, total)


def whole(operand, around):
    array, index = operand
    start, length = around
    members = array.shape[-1]
    k = start // length
    if index is None:
        return pl.BlockSpec((array.shape[0], length, members), lambda j: (0, k, 0))
    return pl.BlockSpec((array.shape[0], None, length, members), lambda j: (0, index, k, 0))


def edge(operand):
    array, index = operand
    if index is None:
        return pl.BlockSpec(array.shape, lambda j: (0, 0))
    return pl.BlockSpec((None, *array.shape[1:]), lambda j: (index, 0, 0))


def updated_row(refs, start, j, piece):
    mid, low, up, before, speed, k_low, k_high, j_low, j_high = refs
    rows = mid.shape[0]
    first, size = piece
    own = pl.ds(first - window(piece, j_low.shape[0])[0], size)
    line = pl.ds(first, size)
    row = start + j
    here = mid[row]
    length = here.shape[0]
    part = slice(own.start, own.start + size)
    position = lax.broadcasted_iota(jnp.int32, here.shape, 0)
    earlier_j = jnp.where(row == 0, j_low[line, :], mid[jnp.maximum(row - 1, 0), own, :])
    later_j = jnp.where(row == rows - 1, j_high[line, :], mid[jnp.minimum(row + 1, rows - 1), own, :])
    lower_k = jnp.where(position == 0, k_low[pl.ds(row, 1), :], pltpu.roll(here, 1, 0))[part]
    upper_k = jnp.where(position == length - 1, k_high[pl.ds(row, 1), :], pltpu.roll(here, length - 1, 0))[part]
    here = here[part]
    spread = earlier_j + later_j + low[j] + up[j] + lower_k + upper_k - 6.0 * here
    return 2.0 * here - before[j] + speed[j] * spread


def step_kernel(*refs, rows, piece):
    ins, (out, k_first, k_last, j_first, j_last) = refs[:9], refs[9:]
    block = pl.program_id(0)
    start = block * rows

    def body(j, carry):
        new = updated_row(ins, start, j, piece)
        out[j] = new
        k_first[pl.ds(j, 1), :] = new[:1]
        k_last[pl.ds(j, 1), :] = new[new.shape[0] - 1 :]
        return carry

    lax.fori_loop(0, rows, body, 0, unroll=4)

    @pl.when(block == 0)
    def _():
        j_first[...] = out[0]

    @pl.when(block == pl.num_programs(0) - 1)
    def _():
        j_last[...] = out[rows - 1]


def last_kernel(*refs, rows, piece, aliased):
    ins = refs[:9]
    out, field, stats, guess, total, square = refs[9 + aliased :]
    block = pl.program_id(0)
    start = block * rows

    @pl.when(block == 0)
    def _():
        guess[...] = updated_row(ins, start, 0, piece)
        total[...] = jnp.zeros_like(total)
        square[...] = jnp.zeros_like(square)

    base = guess[...]

    def body(j, carry):
        sums, squares = carry
        new = updated_row(ins, start, j, piece)
        out[j] = new
        field[j] = new
        moved = new - base
        return sums + moved, squares + moved * moved

    sums, squares = lax.fori_loop(0, rows, body, (total[...], square[...]), unroll=4)
    total[...] = sums
    square[...] = squares

    @pl.when(block == pl.num_programs(0) - 1)
    def _():
        count = rows * pl.num_programs(0)
        mean = sums / count
        stats[0] = base + mean
        stats[1] = jnp.maximum(squares - sums * mean, 0.0)


def scale_kernel(*refs):
    values, mean, factor = refs[:3]
    out = refs[-1]

    def body(j, carry):
        out[j] = (values[j] - mean[...]) * factor[...]
        return carry

    lax.fori_loop(0, values.shape[0], body, 0, unroll=4)


def cost(microseconds):
    return pl.CostEstimate(flops=int(microseconds * 1.0e9), bytes_accessed=12 << 20, transcendentals=0)


def plane_specs(mid, low, up, before, speed, edges, rows, piece):
    operands = [mid, low, up, before, speed, *edges]
    specs = [whole(mid, window(piece, mid[0].shape[-2]))] + [blocked(o, rows, piece) for o in operands[1:5]] + [edge(o) for o in edges]
    return [array for array, _ in operands], specs


def plane_step(name, mid, low, up, before, speed, edges):
    nj, nk, members = mid[0].shape[0], *mid[0].shape[-2:]
    rows = block_rows(nj)
    arrays, specs = plane_specs(mid, low, up, before, speed, edges, rows, (0, nk))
    plane = pl.BlockSpec((rows, nk, members), lambda j: (j, 0, 0))
    k_edge = pl.BlockSpec((rows, members), lambda j: (j, 0))
    j_edge = pl.BlockSpec((nk, members), lambda j: (0, 0))
    shape = functools.partial(jax.ShapeDtypeStruct, dtype=jnp.float32)
    return pl.pallas_call(
        functools.partial(step_kernel, rows=rows, piece=(0, nk)),
        grid=(nj // rows,),
        in_specs=specs,
        out_specs=[plane, k_edge, k_edge, j_edge, j_edge],
        out_shape=[shape((nj, nk, members)), shape((nj, members)), shape((nj, members)), shape((nk, members)), shape((nk, members))],
        cost_estimate=cost(8),
        name=name,
    )(*arrays)


def plane_last(name, mid, low, up, before, speed, edges, field, index, field_shape, piece):
    nj, members = mid[0].shape[0], mid[0].shape[-1]
    first, nk = piece
    k = first // nk
    rows = block_rows(nj)
    arrays, specs = plane_specs(mid, low, up, before, speed, edges, rows, piece)
    shape = functools.partial(jax.ShapeDtypeStruct, dtype=jnp.float32)
    aliases = {}
    if field is not None:
        aliases = {len(arrays): 1}
        arrays.append(field)
        specs.append(pl.BlockSpec(memory_space=pl.ANY))
    return pl.pallas_call(
        functools.partial(last_kernel, rows=rows, piece=piece, aliased=len(aliases)),
        grid=(nj // rows,),
        in_specs=specs,
        out_specs=[
            pl.BlockSpec((rows, nk, members), lambda j: (j, 0, 0)),
            pl.BlockSpec((rows, None, nk, members), lambda j: (j, index, k, 0)),
            pl.BlockSpec((2, nk, members), lambda j: (0, 0, 0)),
        ],
        out_shape=[shape((nj, nk, members)), shape(field_shape), shape((2, nk, members))],
        scratch_shapes=[pltpu.VMEM((nk, members), jnp.float32)] * 3,
        input_output_aliases=aliases,
        cost_estimate=cost(8),
        name=name,
    )(*arrays)


def plane_scale(name, values, mean, factor, scaled, index, field_shape, piece):
    nj, nk, members = values.shape
    k = piece[0] // nk
    rows = block_rows(nj)
    arrays = [values, mean, factor]
    line = pl.BlockSpec((nk, members), lambda j: (0, 0))
    specs = [pl.BlockSpec((rows, nk, members), lambda j: (j, 0, 0)), line, line]
    aliases = {}
    if scaled is not None:
        aliases = {3: 0}
        arrays.append(scaled)
        specs.append(pl.BlockSpec(memory_space=pl.ANY))
    return pl.pallas_call(
        scale_kernel,
        grid=(nj // rows,),
        in_specs=specs,
        out_specs=pl.BlockSpec((rows, None, nk, members), lambda j: (j, index, k, 0)),
        out_shape=jax.ShapeDtypeStruct(field_shape, jnp.float32),
        input_output_aliases=aliases,
        cost_estimate=cost(4),
        name=name,
    )(*arrays)


def exchanged(k_first, k_last, j_first, j_last):
    return (shift(k_last, "slabs", 1), shift(k_first, "slabs", -1), shift(j_last, "rows", 1), shift(j_first, "rows", -1))


def line_factors(stats, local):
    count = lax.axis_size("rows")
    parts = [stats] + [shift(stats, "rows", by) for by in range(1, count)]
    mean = sum(part[..., 0, :, :] for part in parts) / count
    spread = sum(part[..., 1, :, :] for part in parts) / (local * count)
    spread = spread + sum((part[..., 0, :, :] - mean) ** 2 for part in parts) / count
    return mean, lax.rsqrt(spread + 0.0001)


def shards(pressure, earlier, speed_square):
    nj, ni, nk, members = pressure.shape
    top = ni - 1
    inner = range(1, top)
    now = [(pressure, i) for i in range(ni)]
    before = [(earlier, i) for i in range(ni)]
    speed = [(speed_square, i) for i in range(ni)]
    face = pressure[:, top]
    face, behind = lax.optimization_barrier((face, pressure))
    first_top = shift(face, "cols", 1)
    swap = lambda values: jnp.transpose(values, (1, 0, 2))
    halos = exchanged(swap(pressure[:, :, 0]), swap(pressure[:, :, nk - 1]), pressure[0], pressure[nj - 1])
    received = {"low": first_top, "up": shift(behind[:, 0], "cols", -1)}
    edges = [[(h, i) for h in halos] for i in range(ni)]
    for step in range(STEPS - 1):
        order = (0, top) if step % 2 == 0 else (top, 0)
        later, new_edges, arriving = [None] * ni, [None] * ni, {}
        ready = [None] * ni

        def compute(i):
            low = (received["low"], None) if i == 0 else now[i - 1]
            up = (received["up"], None) if i == top else now[i + 1]
            ready[i] = plane_step(f"step{step}_plane{i}", now[i], low, up, before[i], speed[i], edges[i])
            later[i] = (ready[i][0], None)

        for i in inner:
            compute(i)
        stacked = exchanged(*[jnp.stack([ready[i][n] for i in inner]) for n in range(1, 5)])
        for i in inner:
            new_edges[i] = [(h, i - 1) for h in stacked]
        for i in order:
            compute(i)
            side, by = ("up", -1) if i == 0 else ("low", 1)
            if step == STEPS - 2 and i == order[1]:
                arriving[side] = [shift(ready[i][0][:, first : first + size], "cols", by) for first, size in pieces(nk)]
            else:
                arriving[side] = shift(ready[i][0], "cols", by)
            new_edges[i] = [(h, None) for h in exchanged(*ready[i][1:])]
        before, now, edges, received = now, later, new_edges, arriving
    order = (0, top) if STEPS % 2 == 1 else (top, 0)
    field = scaled = None
    full = (0, nk)

    def finish(i, low, up, piece):
        return plane_last(f"last_plane{i}_{piece[0]}", now[i], low, up, before[i], speed[i], edges[i], field, i, pressure.shape, piece)

    done = []
    for i in inner:
        values, field, stats = finish(i, now[i - 1], now[i + 1], full)
        done.append((values, stats))
    mean, factor = line_factors(jnp.stack([stats for _, stats in done]), nj)
    for i in inner:
        scaled = plane_scale(f"scale_plane{i}", done[i - 1][0], mean[i - 1], factor[i - 1], scaled, i, pressure.shape, full)
    for i in order:
        side = "low" if i == 0 else "up"
        arrived = [(received[side], full)] if i == order[0] else list(zip(received[side], pieces(nk)))
        for face, piece in arrived:
            face, scaled = lax.optimization_barrier((face, scaled))
            low = (face, None) if i == 0 else now[i - 1]
            up = (face, None) if i == top else now[i + 1]
            values, field, stats = finish(i, low, up, piece)
            mean, factor = line_factors(stats, nj)
            scaled = plane_scale(f"scale_plane{i}_{piece[0]}", values, mean, factor, scaled, i, pressure.shape, piece)
    return (scaled, field)


def solution(mesh):
    spec = P("rows", "cols", "slabs", None)
    return jax.shard_map(shards, mesh=mesh, in_specs=(spec,) * 3, out_specs=(spec,) * 2, check_vma=False)
```
